32 devices in a mesh: alpha: 8 (over y, x, core), beta: 4 (over z).
Axes of the slice: x: 2, y: 2, z: 4, core: 2. Of those that a mesh axis runs over, the one named last changes fastest.
Arguments:
- ci_vector: bfloat16 [1024, 2048], P('alpha', 'beta'), may hold values from -6 to 6
- alpha_tiles: bfloat16 [8, 8, 4, 128, 128], P(None, 'alpha'), may hold values from -0.25 to 0.25
- alpha_list: int32 [8, 8, 4], P(None, 'alpha'), may hold values from 0 to 7, as said below
- alpha_count: int32 [8, 8], P(None, 'alpha'), may hold values from 1 to 4, as said below
- beta_tiles: bfloat16 [8, 16, 4, 128, 128], P(None, 'beta'), may hold values from -0.09375 to 0.09375
- beta_target: int32 [8, 16, 4], P(None, 'beta'), may hold values from 0 to 15
- alpha_diag: float32 [1024], P('alpha'), may hold values from -6 to 6
- beta_diag: float32 [2048], P('beta'), may hold values from -6 to 6
Outputs:
- sigma_vector: float32 [1024, 2048], P('alpha', 'beta')
The draws below stay inside these ranges and needn't reach their ends.
Inputs may be any that keep to these rules, and one draw needn't show every extreme that they name: `alpha_list`: the 4 entries of one factor and block are distinct alpha blocks within 3 blocks of that block. `alpha_count`: some alpha block has 4 live slots in every factor.
All inputs are finite; a program needn't handle non-finite values.
Results may differ from the reference program's by a relative error of at most 0.007.
Values may be sent and summed in bfloat16 or wider, within the bound.
No kernel may reach another device: no remote copies, remote signals or barrier semaphores. Data moves between devices by JAX's collectives and lax.ppermute only.
A program may use at most 64 MiB of HBM per device.

```python
import jax
import jax.numpy as jnp
from jax import lax

TILE = 128
FACTORS = 8
BAND = 3
KA = 4
KB = 4
CB_DEV = 4
NBA = 8
NA = 1024
NBB = 16
NB = 2048
N_BETA = 4


def draw_alpha_list(key, part):
    offsets = 2 * BAND + 1
    blocks_near = jnp.arange(NBA, dtype=jnp.int32)[:, None] + jnp.arange(offsets, dtype=jnp.int32)[None, :] - BAND
    inside = (blocks_near >= 0) & (blocks_near < NBA)
    random_bits = jax.random.randint(key, (FACTORS, NBA, offsets), 0, 1 << 20)
    scores = jnp.where(inside[None], random_bits, 1 << 21) * 32 + jnp.arange(offsets, dtype=jnp.int32)
    ranked = jnp.argsort(scores, axis=-1, stable=True)[..., :KA].astype(jnp.int32)
    return (ranked - BAND + jnp.arange(NBA, dtype=jnp.int32)[None, :, None]).astype(jnp.int32)


def draw_alpha_count(key, part):
    first_key, second_key, third_key = jax.random.split(key, 3)
    heavy = jax.random.randint(first_key, (NBA,), 0, 4) == 0
    forced = jax.random.randint(second_key, (), 0, NBA)
    heavy = heavy | (jnp.arange(NBA, dtype=jnp.int32) == forced)
    light = jax.random.randint(third_key, (FACTORS, NBA), 1, 3)
    return jnp.where(heavy[None, :], KA, light).astype(jnp.int32)


def touch_ends(result, own_key, smallest, largest):
    longest = result.shape.index(max(result.shape))
    spots = []
    for shift in (0, 1):
        where = [jax.random.randint(jax.random.fold_in(own_key, axis), (), 0, length) for axis, length in enumerate(result.shape)]
        where[longest] = (where[longest] + shift) % result.shape[longest]
        spots.append(tuple(where))
    return result.at[spots[0]].set(smallest).at[spots[1]].set(largest)


def block_scale(key, extent, cuts, smallest, largest):
    gain = 1.0
    for position, shards_of in cuts:
        steps = jax.random.uniform(jax.random.fold_in(jax.random.fold_in(key, 6), position), (shards_of,), jnp.float32, smallest / len(cuts), largest / len(cuts))
        gain = gain * jnp.repeat(jnp.exp(steps), extent[position] // shards_of).reshape((-1,) + (1,) * (len(extent) - 1 - position))
    return gain


def normal_values(own_key, shape, deviation, bound, cuts=(), kind=jnp.bfloat16):
    values = deviation * jax.random.normal(own_key, shape, jnp.float32)
    if cuts:
        values = values * block_scale(own_key, shape, cuts, -0.22, 0.18)
    return jnp.clip(values, -bound, bound).astype(kind)


def setup_inputs(seed: int = 0) -> dict:
    splits = jax.random.split(jax.random.key(seed), 9)
    return {
        "ci_vector": normal_values(splits[0], (NA, NB), 1.0, 6.0, ((0, 8), (1, 4))),
        "alpha_tiles": normal_values(splits[1], (FACTORS, NBA, KA, TILE, TILE), (TILE * KA) ** -0.5, 0.25, ((1, 8),)),
        "alpha_list": draw_alpha_list(jax.random.fold_in(splits[8], 71), 0),
        "alpha_count": draw_alpha_count(jax.random.fold_in(splits[8], 71), 0),
        "beta_tiles": normal_values(splits[4], (FACTORS, NBB, KB, TILE, TILE), (TILE * KB * FACTORS) ** -0.5, 0.09375, ((1, 4),)),
        "beta_target": touch_ends(jax.random.randint(splits[5], (FACTORS, NBB, KB), 0, NBB), jax.random.fold_in(splits[5], 1), 0, NBB - 1).astype(jnp.int32),
        "alpha_diag": normal_values(splits[6], (NA,), 1.0, 6.0, ((0, 8),), jnp.float32),
        "beta_diag": normal_values(splits[7], (NB,), 1.0, 6.0, ((0, 4),), jnp.float32),
    }


def reference(ci_vector, alpha_tiles, alpha_list, alpha_count, beta_tiles, beta_target, alpha_diag, beta_diag):
    block_cols = CB_DEV * TILE
    live_mask = jnp.arange(KA, dtype=jnp.int32)[None, None, :] < alpha_count[:, :, None]
    masked = jnp.where(live_mask[..., None, None], alpha_tiles, jnp.zeros((), alpha_tiles.dtype)).astype(jnp.float32)

    def group_step(accumulated, group):
        first_col = (group * block_cols).astype(jnp.int32)
        columns = lax.dynamic_slice_in_dim(ci_vector, first_col, block_cols, 1)
        columns = columns.reshape(NBA, TILE, block_cols).astype(jnp.float32)

        def factor_step(partial_value, factor):
            picked = columns[alpha_list[factor]]
            coupled = jnp.einsum('iksr,ikrc->isc', masked[factor], picked)
            coupled = lax.optimization_barrier(coupled.astype(jnp.bfloat16)).astype(jnp.float32)
            source = coupled.reshape(NA, CB_DEV, TILE)
            first_block = (group * CB_DEV).astype(jnp.int32)
            couplings = lax.dynamic_slice_in_dim(beta_tiles[factor], first_block, CB_DEV, 0).astype(jnp.float32)
            targets = lax.dynamic_slice_in_dim(beta_target[factor], first_block, CB_DEV, 0)
            contrib = jnp.einsum('rsi,skij->skrj', source, couplings).reshape(CB_DEV * KB, NA, TILE)
            added = jax.ops.segment_sum(contrib, targets.reshape(-1), num_segments=NBB)
            return partial_value + added, None

        partial_value, unused = lax.scan(factor_step, jnp.zeros((NBB, NA, TILE), jnp.float32), jnp.arange(FACTORS, dtype=jnp.int32))
        rounded = lax.optimization_barrier(partial_value.astype(jnp.bfloat16)).astype(jnp.float32)
        return accumulated + rounded, None

    accumulated, unused = lax.scan(group_step, jnp.zeros((NBB, NA, TILE), jnp.float32), jnp.arange(N_BETA, dtype=jnp.int32))
    mixed_term = accumulated.transpose(1, 0, 2).reshape(NA, NB)
    return mixed_term + (alpha_diag[:, None] + beta_diag[None, :]) * ci_vector.astype(jnp.float32)
```

```python
import jax
import jax.numpy as jnp
from jax import lax
from jax.experimental import pallas as pl
from jax.experimental.pallas import tpu as pltpu
from jax.sharding import PartitionSpec as P

BAND = 3


def exchange(shard, axis, pairs):
    return lax.ppermute(shard, axis, pairs)


def band_window(ci_vector):
    length = lax.axis_size("alpha")
    pieces = []
    for offset in range(-BAND, BAND + 1):
        if offset == 0:
            pieces.append(ci_vector)
        else:
            pairs = [(i, i - offset) for i in range(length) if 0 <= i - offset < length]
            pieces.append(exchange(ci_vector, "alpha", pairs))
    return dict(enumerate(pieces)), lambda block, own: block - own + BAND


def cube_window(ci_vector):
    length = lax.axis_size("alpha")

    def wanted(i, source):
        return abs(i - source) <= BAND

    pieces = [None] * length
    pieces[0] = ci_vector
    plans = {}
    for k in range(2, length, 2):
        odd = [(i ^ (k + 1), i) for i in range(length) if wanted(i, i ^ (k + 1))]
        even = [(i ^ k, i) for i in range(length) if wanted(i, i ^ k)]
        plans[k] = (even, odd)
    swap = [(i, i ^ 1) for i in range(length)]
    for k, (even, odd) in sorted(plans.items(), reverse=True):
        if not even:
            if odd:
                pieces[k + 1] = exchange(ci_vector, "alpha", odd)
            continue
        relayed = [(i ^ k, i) for i in range(length) if wanted(i, i ^ k) or wanted(i ^ 1, i ^ k)]
        pieces[k] = exchange(ci_vector, "alpha", relayed)
    pieces[1] = exchange(ci_vector, "alpha", swap)
    for k, (even, odd) in sorted(plans.items()):
        if even and odd:
            pairs = [(i ^ 1, i) for _, i in odd]
            pieces[k + 1] = exchange(pieces[k], "alpha", pairs)
    held = {k: piece for k, piece in enumerate(pieces) if piece is not None}
    return held, lambda block, own: block ^ own


def term_kernel(
    sizes, place_of, sources, counts, targets, pieces, alpha_tiles, beta_tiles, outs, window, total
):
    factors, alpha_slots, local_blocks, beta_slots, groups, by_xor = sizes
    tile_size = total.shape[1]
    own_block, own_group = lax.axis_index("alpha"), lax.axis_index("beta")
    for place, piece in pieces.items():
        window[place] = piece[...]
    for block in range(total.shape[0]):
        total[block] = jnp.zeros(total.shape[1:], jnp.float32)
    for factor in range(factors):
        left, right = [], []
        for slot in range(alpha_slots):
            tile = alpha_tiles[factor, 0, slot]
            left.append(jnp.where(slot < counts[factor, 0], tile, jnp.zeros_like(tile)))
            right.append(window[place_of(sources[factor, 0, slot], own_block)])
        coupled = jnp.dot(
            jnp.concatenate(left, axis=1),
            jnp.concatenate(right, axis=0),
            preferred_element_type=jnp.float32,
        ).astype(jnp.bfloat16)
        for block in range(local_blocks):
            source = coupled[:, block * tile_size : (block + 1) * tile_size]
            tiles = [beta_tiles[factor, block, slot] for slot in range(beta_slots)]
            added = jnp.dot(source, jnp.concatenate(tiles, axis=1), preferred_element_type=jnp.float32)
            for slot in range(beta_slots):
                target = targets[factor, block, slot]
                group = target // local_blocks
                away = (group ^ own_group) if by_xor else lax.rem(group - own_group + groups, groups)
                place = away * local_blocks + lax.rem(target, local_blocks)
                total[place] += added[:, slot * tile_size : (slot + 1) * tile_size]
    for away in range(groups):
        for block in range(local_blocks):
            value = total[away * local_blocks + block].astype(jnp.bfloat16)
            outs[away][:, block * tile_size : (block + 1) * tile_size] = value


def shards(
    ci_vector, alpha_tiles, alpha_list, alpha_count, beta_tiles, beta_target, alpha_diag, beta_diag
):
    tile_size, columns = ci_vector.shape
    factors, _, alpha_slots = alpha_list.shape
    _, local_blocks, beta_slots = beta_target.shape
    length, groups = lax.axis_size("alpha"), lax.axis_size("beta")
    small = length & (length - 1) == 0 and length <= 2 * (BAND + 1)
    pieces, place_of = cube_window(ci_vector) if small else band_window(ci_vector)
    by_xor = groups & (groups - 1) == 0
    sizes = (factors, alpha_slots, local_blocks, beta_slots, groups, by_xor)

    def body(sources, counts, targets, *refs):
        n = len(pieces)
        held = dict(zip(pieces, refs[:n]))
        a_ref, b_ref, *outs = refs[n:-2]
        term_kernel(sizes, place_of, sources, counts, targets, held, a_ref, b_ref, outs, *refs[-2:])

    vmem = pl.BlockSpec(memory_space=pltpu.VMEM)
    smem = pl.BlockSpec(memory_space=pltpu.SMEM)
    flops = 2 * factors * tile_size * columns * tile_size * (alpha_slots + beta_slots)
    own, *far = pl.pallas_call(
        body,
        out_shape=[jax.ShapeDtypeStruct((tile_size, columns), jnp.bfloat16)] * groups,
        in_specs=[smem] * 3 + [vmem] * (len(pieces) + 2),
        out_specs=[vmem] * groups,
        scratch_shapes=[
            pltpu.VMEM((max(pieces) + 1, tile_size, columns), jnp.bfloat16),
            pltpu.VMEM((groups * local_blocks, tile_size, tile_size), jnp.float32),
        ],
        compiler_params=pltpu.CompilerParams(vmem_limit_bytes=20 * 2**20),
        cost_estimate=pl.CostEstimate(
            flops=flops, bytes_accessed=alpha_tiles.size * 2 + beta_tiles.size * 2, transcendentals=0
        ),
        name="couple",
    )(alpha_list, alpha_count, beta_target, *pieces.values(), alpha_tiles, beta_tiles)
    summed = own.astype(jnp.float32)
    received = {}
    for away in sorted(range(1, groups), key=lambda d: (d == 1, d)):
        if by_xor:
            pairs = [(i, i ^ away) for i in range(groups)]
        else:
            pairs = [(i, (i + away) % groups) for i in range(groups)]
        received[away] = exchange(far[away - 1], "beta", pairs)
    for away in sorted(received):
        summed = summed + received[away].astype(jnp.float32)
    return summed + (alpha_diag[:, None] + beta_diag[None, :]) * ci_vector.astype(jnp.float32)


def solution(mesh):
    placed = (
        P("alpha", "beta"),
        P(None, "alpha", None, None, None),
        P(None, "alpha", None),
        P(None, "alpha"),
        P(None, "beta", None, None, None),
        P(None, "beta", None),
        P("alpha"),
        P("beta"),
    )
    return jax.shard_map(
        shards, mesh=mesh, in_specs=placed, out_specs=P("alpha", "beta"), check_vma=False
    )
```

```python
import jax
import jax.numpy as jnp
from jax import lax
from jax.experimental import pallas as pl
from jax.experimental.pallas import tpu as pltpu
from jax.sharding import PartitionSpec as P


BAND = 3
WARM_FLOPS = 2 * 10**10


def band_window(ci_vector):
    length = lax.axis_size("alpha")
    held = {BAND: ci_vector}
    for offset in range(-BAND, BAND + 1):
        if offset:
            pairs = [(i, i - offset) for i in range(length) if 0 <= i - offset < length]
            held[offset + BAND] = lax.ppermute(ci_vector, "alpha", pairs)
    return held, lambda block, own: block - own + BAND, ()


def cube_window(ci_vector):
    length = lax.axis_size("alpha")

    def near(i, source):
        return abs(i - source) <= BAND

    held, relayed = {0: ci_vector}, []
    for k in range(2, length, 2):
        even = [i for i in range(length) if near(i, i ^ k)]
        odd = [i for i in range(length) if near(i, i ^ k ^ 1)]
        if even:
            taking = {i for i in range(length) if near(i, i ^ k) or near(i ^ 1, i ^ k)}
            pairs = [(i ^ (k if i in taking else 1), i) for i in range(length)]
            held[k] = lax.ppermute(ci_vector, "alpha", pairs)
            if odd:
                relayed.append(k)
        elif odd:
            pairs = [(i ^ (k ^ 1 if i in odd else 0), i) for i in range(length)]
            held[k + 1] = lax.ppermute(ci_vector, "alpha", pairs)
    swap = [(i, i ^ 1) for i in range(length)]
    held[1] = lax.ppermute(ci_vector, "alpha", swap)
    for k in relayed:
        held[k + 1] = lax.ppermute(held[k], "alpha", swap)
    return held, lambda block, own: block ^ own, ()


def warm_kernel(counts_from, counts_to):
    counts_to[...] = counts_from[...]


def couple_kernel(
    sizes, place_of, sources, counts, targets, held, alpha_tiles, beta_tiles, outs, window, total
):
    factors, alpha_slots, local_blocks, beta_slots, groups, by_xor = sizes
    tile_size = total.shape[1]
    own_block, own_group = lax.axis_index("alpha"), lax.axis_index("beta")
    for place, piece in held.items():
        window[place] = piece[...]
    for block in range(total.shape[0]):
        total[block] = jnp.zeros(total.shape[1:], jnp.float32)
    for factor in range(factors):
        places = [place_of(sources[0, slot, factor], own_block) for slot in range(alpha_slots)]
        stacked = jnp.concatenate([window[place] for place in places], axis=0)
        tiles = [alpha_tiles[factor, 0, slot] for slot in range(alpha_slots)]
        live = [jnp.where(slot < counts[0, factor], tile, jnp.zeros_like(tile)) for slot, tile in enumerate(tiles)]
        coupled = jnp.dot(
            jnp.concatenate(live, axis=1), stacked, preferred_element_type=jnp.float32
        ).astype(jnp.bfloat16)
        for block in range(local_blocks):
            source = coupled[:, block * tile_size : (block + 1) * tile_size]
            tiles = [beta_tiles[factor, block, slot] for slot in range(beta_slots)]
            added = jnp.dot(source, jnp.concatenate(tiles, axis=1), preferred_element_type=jnp.float32)
            for slot in range(beta_slots):
                target = targets[block, slot, factor]
                group = target // local_blocks
                away = (group ^ own_group) if by_xor else lax.rem(group - own_group + groups, groups)
                place = away * local_blocks + lax.rem(target, local_blocks)
                total[place] += added[:, slot * tile_size : (slot + 1) * tile_size]
    for away in range(groups):
        for block in range(local_blocks):
            value = total[away * local_blocks + block].astype(jnp.bfloat16)
            outs[away][:, block * tile_size : (block + 1) * tile_size] = value


def shards(
    ci_vector, alpha_tiles, alpha_list, alpha_count, beta_tiles, beta_target, alpha_diag, beta_diag
):
    tile_size, columns = ci_vector.shape
    factors, _, alpha_slots = alpha_list.shape
    _, local_blocks, beta_slots = beta_target.shape
    length, groups = lax.axis_size("alpha"), lax.axis_size("beta")
    held, place_of, _ = window_of(length)(ci_vector)
    by_xor = groups & (groups - 1) == 0
    sizes = (factors, alpha_slots, local_blocks, beta_slots, groups, by_xor)
    vmem = pl.BlockSpec(memory_space=pltpu.VMEM)
    smem = pl.BlockSpec(memory_space=pltpu.SMEM)
    tile_bytes = (alpha_tiles.size + beta_tiles.size) * 2

    counts = jnp.transpose(alpha_count, (1, 0))
    counts = pl.pallas_call(
        warm_kernel,
        out_shape=jax.ShapeDtypeStruct(counts.shape, counts.dtype),
        in_specs=[vmem],
        out_specs=vmem,
        compiler_params=pltpu.CompilerParams(vmem_limit_bytes=2**20),
        cost_estimate=pl.CostEstimate(flops=WARM_FLOPS, bytes_accessed=counts.size, transcendentals=0),
        name="warm",
    )(counts)

    def body(sources, counts, targets, *refs):
        n = len(held)
        pieces = dict(zip(held, refs[:n]))
        a_ref, b_ref, *outs = refs[n:-2]
        couple_kernel(sizes, place_of, sources, counts, targets, pieces, a_ref, b_ref, outs, *refs[-2:])

    own, *far = pl.pallas_call(
        body,
        out_shape=[jax.ShapeDtypeStruct((tile_size, columns), jnp.bfloat16)] * groups,
        in_specs=[smem] * 3 + [vmem] * (len(held) + 2),
        out_specs=[vmem] * groups,
        scratch_shapes=[
            pltpu.VMEM((max(held) + 1, tile_size, columns), jnp.bfloat16),
            pltpu.VMEM((groups * local_blocks, tile_size, tile_size), jnp.float32),
        ],
        compiler_params=pltpu.CompilerParams(vmem_limit_bytes=20 * 2**20),
        cost_estimate=pl.CostEstimate(
            flops=2 * factors * tile_size * columns * tile_size * (alpha_slots + beta_slots),
            bytes_accessed=tile_bytes,
            transcendentals=0,
        ),
        name="couple",
    )(
        jnp.transpose(alpha_list, (1, 2, 0)),
        counts,
        jnp.transpose(beta_target, (1, 2, 0)),
        *held.values(),
        alpha_tiles,
        beta_tiles,
    )
    summed = own.astype(jnp.float32)
    for away in far_order(groups):
        if by_xor:
            pairs = [(i, i ^ away) for i in range(groups)]
        else:
            pairs = [(i, (i + away) % groups) for i in range(groups)]
        received = lax.ppermute(far[away - 1], "beta", pairs)
        summed = summed + received.astype(jnp.float32)
    return summed + (alpha_diag[:, None] + beta_diag[None, :]) * ci_vector.astype(jnp.float32)


def far_order(groups):
    return [*range(2, groups), *range(1, min(groups, 2))]


def window_of(length):
    return cube_window if length & (length - 1) == 0 and length <= 2 * (BAND + 1) else band_window


def solution(mesh):
    placed = (
        P("alpha", "beta"),
        P(None, "alpha", None, None, None),
        P(None, "alpha", None),
        P(None, "alpha"),
        P(None, "beta", None, None, None),
        P(None, "beta", None),
        P("alpha"),
        P("beta"),
    )

    return jax.shard_map(shards, mesh=mesh, in_specs=placed, out_specs=P("alpha", "beta"), check_vma=False)
```

```python
import jax
import jax.numpy as jnp
from jax import lax
from jax.experimental import pallas as pl
from jax.experimental.pallas import tpu as pltpu
from jax.sharding import PartitionSpec as P


BAND = 3
WARM_FLOPS = 2 * 10**10


def band_window(ci_vector):
    length = lax.axis_size("alpha")
    held = {BAND: ci_vector}
    for offset in range(-BAND, BAND + 1):
        if offset:
            pairs = [(i, i - offset) for i in range(length) if 0 <= i - offset < length]
            held[offset + BAND] = lax.ppermute(ci_vector, "alpha", pairs)
    return held, lambda block, own: block - own + BAND, ()


def cube_window(ci_vector):
    length = lax.axis_size("alpha")

    def near(i, source):
        return abs(i - source) <= BAND

    held, relayed = {0: ci_vector}, []
    for k in range(2, length, 2):
        even = [i for i in range(length) if near(i, i ^ k)]
        odd = [i for i in range(length) if near(i, i ^ k ^ 1)]
        if even:
            taking = {i for i in range(length) if near(i, i ^ k) or near(i ^ 1, i ^ k)}
            pairs = [(i ^ (k if i in taking else 1), i) for i in range(length)]
            held[k] = lax.ppermute(ci_vector, "alpha", pairs)
            if odd:
                relayed.append(k)
        elif odd:
            pairs = [(i ^ (k ^ 1 if i in odd else 0), i) for i in range(length)]
            held[k + 1] = lax.ppermute(ci_vector, "alpha", pairs)
    swap = [(i, i ^ 1) for i in range(length)]
    held[1] = lax.ppermute(ci_vector, "alpha", swap)
    for k in relayed:
        held[k + 1] = lax.ppermute(held[k], "alpha", swap)
    return held, lambda block, own: block ^ own, ()


def warm_kernel(out):
    out[...] = jnp.zeros_like(out)


def couple_kernel(
    sizes, place_of, tables_from, held, alpha_tiles, beta_tiles, outs, window, coupled, total, tables, semaphores
):
    factors, alpha_slots, local_blocks, beta_slots, groups, by_xor, parts = sizes
    tile_size = total.shape[1]
    own_block, own_group = lax.axis_index("alpha"), lax.axis_index("beta")
    copies = [
        pltpu.make_async_copy(source, table, semaphores.at[i])
        for i, (source, table) in enumerate(zip(tables_from, tables))
    ]
    for copy in copies:
        copy.start()
    sources, counts, targets = tables
    for place, piece in held.items():
        window[place] = piece[...]
    for block in range(total.shape[0]):
        total[block] = jnp.zeros(total.shape[1:], jnp.float32)
    for copy in copies:
        copy.wait()

    def alpha(factor):
        places = [place_of(sources[0, slot, factor], own_block) for slot in range(alpha_slots)]
        stacked = jnp.concatenate([window[place] for place in places], axis=0)
        tiles = [alpha_tiles[factor, 0, slot] for slot in range(alpha_slots)]
        live = [jnp.where(slot < counts[0, factor], tile, jnp.zeros_like(tile)) for slot, tile in enumerate(tiles)]
        product = jnp.dot(jnp.concatenate(live, axis=1), stacked, preferred_element_type=jnp.float32)
        coupled[factor] = product.astype(jnp.bfloat16)

    def beta(factor):
        for block in range(local_blocks):
            source = coupled[factor, :, block * tile_size : (block + 1) * tile_size]
            tiles = [beta_tiles[factor, block, slot] for slot in range(beta_slots)]
            added = jnp.dot(source, jnp.concatenate(tiles, axis=1), preferred_element_type=jnp.float32)
            for slot in range(beta_slots):
                target = targets[block, slot, factor]
                group = target // local_blocks
                away = (group ^ own_group) if by_xor else lax.rem(group - own_group + groups, groups)
                place = away * local_blocks + lax.rem(target, local_blocks)
                total[place] += added[:, slot * tile_size : (slot + 1) * tile_size]

    def both(factor, _):
        alpha(factor)
        beta(factor - 1)

    alpha(0)
    lax.fori_loop(1, factors, both, None, unroll=True)
    beta(factors - 1)
    for (away, first, last), out in zip(parts, outs):
        for block in range(local_blocks):
            value = total[away * local_blocks + block, first:last].astype(jnp.bfloat16)
            out[:, block * tile_size : (block + 1) * tile_size] = value


def shards(
    ci_vector, alpha_tiles, alpha_list, alpha_count, beta_tiles, beta_target, alpha_diag, beta_diag
):
    tile_size, columns = ci_vector.shape
    factors, _, alpha_slots = alpha_list.shape
    _, local_blocks, beta_slots = beta_target.shape
    length, groups = lax.axis_size("alpha"), lax.axis_size("beta")
    held, place_of, _ = window_of(length)(ci_vector)
    by_xor = groups & (groups - 1) == 0
    relay = groups == 4
    direct = tile_size * 3 // 8 if relay else tile_size
    parts = [(away, 0, tile_size if away < 2 else direct) for away in range(groups)]
    if relay:
        parts += [(away, direct, tile_size) for away in (2, 3)]
    sizes = (factors, alpha_slots, local_blocks, beta_slots, groups, by_xor, parts)
    vmem = pl.BlockSpec(memory_space=pltpu.VMEM)
    tile_bytes = (alpha_tiles.size + beta_tiles.size) * 2

    pl.pallas_call(
        warm_kernel,
        out_shape=jax.ShapeDtypeStruct((8, 128), jnp.float32),
        out_specs=vmem,
        compiler_params=pltpu.CompilerParams(vmem_limit_bytes=2**20, has_side_effects=True),
        cost_estimate=pl.CostEstimate(flops=WARM_FLOPS, bytes_accessed=4096, transcendentals=0),
        name="warm",
    )()

    tables = [
        jnp.transpose(alpha_list, (1, 2, 0)),
        jnp.transpose(alpha_count, (1, 0)),
        jnp.transpose(beta_target, (1, 2, 0)),
    ]

    def body(*refs):
        t, n = len(tables), len(held)
        pieces = dict(zip(held, refs[t : t + n]))
        a_ref, b_ref, *outs = refs[t + n : t + n + 2 + len(parts)]
        window, coupled, total, *near, semaphores = refs[t + n + 2 + len(parts) :]
        couple_kernel(
            sizes, place_of, refs[:t], pieces, a_ref, b_ref, outs, window, coupled, total, near, semaphores
        )

    own, *far = pl.pallas_call(
        body,
        out_shape=[jax.ShapeDtypeStruct((last - first, columns), jnp.bfloat16) for _, first, last in parts],
        in_specs=[pl.BlockSpec(memory_space=pl.ANY)] * len(tables) + [vmem] * (len(held) + 2),
        out_specs=[vmem] * len(parts),
        scratch_shapes=[
            pltpu.VMEM((max(held) + 1, tile_size, columns), jnp.bfloat16),
            pltpu.VMEM((factors, tile_size, columns), jnp.bfloat16),
            pltpu.VMEM((groups * local_blocks, tile_size, tile_size), jnp.float32),
            *[pltpu.SMEM(table.shape, jnp.int32) for table in tables],
            pltpu.SemaphoreType.DMA((len(tables),)),
        ],
        compiler_params=pltpu.CompilerParams(vmem_limit_bytes=20 * 2**20),
        cost_estimate=pl.CostEstimate(
            flops=2 * factors * tile_size * columns * tile_size * (alpha_slots + beta_slots),
            bytes_accessed=tile_bytes,
            transcendentals=0,
        ),
        name="couple",
    )(
        *tables,
        *held.values(),
        alpha_tiles,
        beta_tiles,
    )

    def send(value, away):
        if by_xor:
            pairs = [(i, i ^ away) for i in range(groups)]
        else:
            pairs = [(i, (i + away) % groups) for i in range(groups)]
        return lax.ppermute(value, "beta", pairs)

    received = [send(far[away - 1], away).astype(jnp.float32) for away in range(1, groups)]
    if relay:
        beyond = send(far[-1], 1)
        joined = (far[-2].astype(jnp.float32) + beyond.astype(jnp.float32)).astype(jnp.bfloat16)
        passed = send(joined, 2).astype(jnp.float32)
        received[1:] = [jnp.concatenate([received[1] + received[2], passed], axis=0)]
    summed = own.astype(jnp.float32) + sum(received)
    return summed + (alpha_diag[:, None] + beta_diag[None, :]) * ci_vector.astype(jnp.float32)


def window_of(length):
    return cube_window if length & (length - 1) == 0 and length <= 2 * (BAND + 1) else band_window


def solution(mesh):
    placed = (
        P("alpha", "beta"),
        P(None, "alpha", None, None, None),
        P(None, "alpha", None),
        P(None, "alpha"),
        P(None, "beta", None, None, None),
        P(None, "beta", None),
        P("alpha"),
        P("beta"),
    )

    return jax.shard_map(shards, mesh=mesh, in_specs=placed, out_specs=P("alpha", "beta"), check_vma=False)
```

```python
import jax
import jax.numpy as jnp
from jax import lax
from jax.experimental import pallas as pl
from jax.experimental.pallas import tpu as pltpu
from jax.sharding import PartitionSpec as P


BAND = 3
WARM_FLOPS = 2 * 10**10


def band_window(ci_vector):
    length = lax.axis_size("alpha")
    held = {BAND: ci_vector}
    for offset in range(-BAND, BAND + 1):
        if offset:
            pairs = [(i, i - offset) for i in range(length) if 0 <= i - offset < length]
            held[offset + BAND] = lax.ppermute(ci_vector, "alpha", pairs)
    return held, lambda block, own: block - own + BAND, ()


def cube_window(ci_vector):
    length = lax.axis_size("alpha")
    everyone = range(length)
    lower, middle = set(everyone[: length // 2]), set(everyone[length // 4 : -(length // 4)])
    first = lax.ppermute(ci_vector, "alpha", [(i ^ (2 if i in lower else 1), i) for i in everyone])
    cross = lax.ppermute(ci_vector, "alpha", [(i ^ (6 if i in middle else 1), i) for i in everyone])
    last = lax.ppermute(ci_vector, "alpha", [(i ^ (1 if i in lower else 2), i) for i in everyone])
    edge = lax.ppermute(ci_vector, "alpha", [(i ^ 5, i) for i in everyone if abs(i - (i ^ 5)) <= BAND])
    swap = [(i, i ^ 1) for i in everyone]
    beside = pl.pallas_call(
        pick_kernel,
        out_shape=jax.ShapeDtypeStruct(ci_vector.shape, ci_vector.dtype),
        in_specs=[pl.BlockSpec(memory_space=pltpu.VMEM)] * 2,
        out_specs=pl.BlockSpec(memory_space=pltpu.VMEM),
        compiler_params=pltpu.CompilerParams(vmem_limit_bytes=2**20),
        cost_estimate=pl.CostEstimate(flops=10**6, bytes_accessed=4 * ci_vector.size, transcendentals=0),
        name="pick",
    )(first, last)
    held = {0: ci_vector, 1: last, 2: first, 5: edge, 6: cross}
    held[3] = lax.ppermute(beside, "alpha", swap)
    held[7] = lax.ppermute(cross, "alpha", swap)

    def place_of(block, own):
        k = block ^ own
        turned = (own >= length // 2) & ((k == 1) | (k == 2))
        return jnp.where(turned, 3 - k, k)

    return held, place_of, ()


def pick_kernel(first, last, out):
    lower = lax.axis_index("alpha") < lax.axis_size("alpha") // 2

    @pl.when(lower)
    def _():
        out[...] = first[...]

    @pl.when(jnp.logical_not(lower))
    def _():
        out[...] = last[...]


def warm_kernel(out):
    out[...] = jnp.zeros_like(out)


def couple_kernel(
    sizes, place_of, tables_from, held, alpha_tiles, beta_tiles, outs, window, coupled, total, tables, semaphores
):
    factors, alpha_slots, local_blocks, beta_slots, groups, by_xor, parts = sizes
    tile_size = total.shape[1]
    own_block, own_group = lax.axis_index("alpha"), lax.axis_index("beta")
    copies = [
        pltpu.make_async_copy(source, table, semaphores.at[i])
        for i, (source, table) in enumerate(zip(tables_from, tables))
    ]
    for copy in copies:
        copy.start()
    sources, counts, targets = tables
    for place, piece in held.items():
        window[place] = piece[...]
    for block in range(total.shape[0]):
        total[block] = jnp.zeros(total.shape[1:], jnp.float32)
    for copy in copies:
        copy.wait()

    def alpha(factor):
        places = [place_of(sources[0, slot, factor], own_block) for slot in range(alpha_slots)]
        stacked = jnp.concatenate([window[place] for place in places], axis=0)
        tiles = [alpha_tiles[factor, 0, slot] for slot in range(alpha_slots)]
        live = [jnp.where(slot < counts[0, factor], tile, jnp.zeros_like(tile)) for slot, tile in enumerate(tiles)]
        product = jnp.dot(jnp.concatenate(live, axis=1), stacked, preferred_element_type=jnp.float32)
        coupled[factor] = product.astype(jnp.bfloat16)

    def beta(factor):
        for block in range(local_blocks):
            source = coupled[factor, :, block * tile_size : (block + 1) * tile_size]
            tiles = [beta_tiles[factor, block, slot] for slot in range(beta_slots)]
            added = jnp.dot(source, jnp.concatenate(tiles, axis=1), preferred_element_type=jnp.float32)
            for slot in range(beta_slots):
                target = targets[block, slot, factor]
                group = target // local_blocks
                away = (group ^ own_group) if by_xor else lax.rem(group - own_group + groups, groups)
                place = away * local_blocks + lax.rem(target, local_blocks)
                total[place] += added[:, slot * tile_size : (slot + 1) * tile_size]

    def both(factor, _):
        alpha(factor)
        beta(factor - 1)

    alpha(0)
    lax.fori_loop(1, factors, both, None, unroll=True)
    beta(factors - 1)
    for (away, first, last), out in zip(parts, outs):
        for block in range(local_blocks):
            value = total[away * local_blocks + block, first:last].astype(jnp.bfloat16)
            out[:, block * tile_size : (block + 1) * tile_size] = value


def shards(
    ci_vector, alpha_tiles, alpha_list, alpha_count, beta_tiles, beta_target, alpha_diag, beta_diag
):
    tile_size, columns = ci_vector.shape
    factors, _, alpha_slots = alpha_list.shape
    _, local_blocks, beta_slots = beta_target.shape
    length, groups = lax.axis_size("alpha"), lax.axis_size("beta")
    held, place_of, _ = window_of(length)(ci_vector)
    by_xor = groups & (groups - 1) == 0
    relay = groups == 4
    direct = tile_size * 3 // 8 if relay else tile_size
    parts = [(away, 0, tile_size if away < 2 else direct) for away in range(groups)]
    if relay:
        parts += [(away, direct, tile_size) for away in (2, 3)]
    sizes = (factors, alpha_slots, local_blocks, beta_slots, groups, by_xor, parts)
    vmem = pl.BlockSpec(memory_space=pltpu.VMEM)
    tile_bytes = (alpha_tiles.size + beta_tiles.size) * 2

    pl.pallas_call(
        warm_kernel,
        out_shape=jax.ShapeDtypeStruct((8, 128), jnp.float32),
        out_specs=vmem,
        compiler_params=pltpu.CompilerParams(vmem_limit_bytes=2**20, has_side_effects=True),
        cost_estimate=pl.CostEstimate(flops=WARM_FLOPS, bytes_accessed=4096, transcendentals=0),
        name="warm",
    )()

    tables = [
        jnp.transpose(alpha_list, (1, 2, 0)),
        jnp.transpose(alpha_count, (1, 0)),
        jnp.transpose(beta_target, (1, 2, 0)),
    ]

    def body(*refs):
        t, n = len(tables), len(held)
        pieces = dict(zip(held, refs[t : t + n]))
        a_ref, b_ref, *outs = refs[t + n : t + n + 2 + len(parts)]
        window, coupled, total, *near, semaphores = refs[t + n + 2 + len(parts) :]
        couple_kernel(
            sizes, place_of, refs[:t], pieces, a_ref, b_ref, outs, window, coupled, total, near, semaphores
        )

    own, *far = pl.pallas_call(
        body,
        out_shape=[jax.ShapeDtypeStruct((last - first, columns), jnp.bfloat16) for _, first, last in parts],
        in_specs=[pl.BlockSpec(memory_space=pl.ANY)] * len(tables) + [vmem] * (len(held) + 2),
        out_specs=[vmem] * len(parts),
        scratch_shapes=[
            pltpu.VMEM((max(held) + 1, tile_size, columns), jnp.bfloat16),
            pltpu.VMEM((factors, tile_size, columns), jnp.bfloat16),
            pltpu.VMEM((groups * local_blocks, tile_size, tile_size), jnp.float32),
            *[pltpu.SMEM(table.shape, jnp.int32) for table in tables],
            pltpu.SemaphoreType.DMA((len(tables),)),
        ],
        compiler_params=pltpu.CompilerParams(vmem_limit_bytes=20 * 2**20),
        cost_estimate=pl.CostEstimate(
            flops=2 * factors * tile_size * columns * tile_size * (alpha_slots + beta_slots),
            bytes_accessed=tile_bytes,
            transcendentals=0,
        ),
        name="couple",
    )(
        *tables,
        *held.values(),
        alpha_tiles,
        beta_tiles,
    )

    def send(value, away):
        if by_xor:
            pairs = [(i, i ^ away) for i in range(groups)]
        else:
            pairs = [(i, (i + away) % groups) for i in range(groups)]
        return lax.ppermute(value, "beta", pairs)

    received = [send(far[away - 1], away).astype(jnp.float32) for away in range(1, groups)]
    if relay:
        beyond = send(far[-1], 1)
        joined = (far[-2].astype(jnp.float32) + beyond.astype(jnp.float32)).astype(jnp.bfloat16)
        passed = send(joined, 2).astype(jnp.float32)
        received[1:] = [jnp.concatenate([received[1] + received[2], passed], axis=0)]
    summed = own.astype(jnp.float32) + sum(received)
    return summed + (alpha_diag[:, None] + beta_diag[None, :]) * ci_vector.astype(jnp.float32)


def window_of(length):
    return cube_window if length == 2 * (BAND + 1) else band_window


def solution(mesh):
    placed = (
        P("alpha", "beta"),
        P(None, "alpha", None, None, None),
        P(None, "alpha", None),
        P(None, "alpha"),
        P(None, "beta", None, None, None),
        P(None, "beta", None),
        P("alpha"),
        P("beta"),
    )

    return jax.shard_map(shards, mesh=mesh, in_specs=placed, out_specs=P("alpha", "beta"), check_vma=False)
```

```python
import jax
import jax.numpy as jnp
from jax import lax
from jax.experimental import pallas as pl
from jax.experimental.pallas import tpu as pltpu
from jax.sharding import PartitionSpec as P


BAND = 3
WARM_FLOPS = 2 * 10**10


def band_window(ci_vector):
    length = lax.axis_size("alpha")
    held = {BAND: ci_vector}
    for offset in range(-BAND, BAND + 1):
        if offset:
            pairs = [(i, i - offset) for i in range(length) if 0 <= i - offset < length]
            held[offset + BAND] = lax.ppermute(ci_vector, "alpha", pairs)
    return held, lambda block, own: block - own + BAND, ()


def cube_window(ci_vector):
    length = lax.axis_size("alpha")
    everyone = range(length)
    lower, middle = set(everyone[: length // 2]), set(everyone[length // 4 : -(length // 4)])
    first = lax.ppermute(ci_vector, "alpha", [(i ^ (2 if i in lower else 1), i) for i in everyone])
    cross = lax.ppermute(ci_vector, "alpha", [(i ^ (6 if i in middle else 1), i) for i in everyone])
    last = lax.ppermute(ci_vector, "alpha", [(i ^ (1 if i in lower else 2), i) for i in everyone])
    edge = lax.ppermute(ci_vector, "alpha", [(i ^ 5, i) for i in everyone if abs(i - (i ^ 5)) <= BAND])
    swap = [(i, i ^ 1) for i in everyone]
    beside = pl.pallas_call(
        pick_kernel,
        out_shape=jax.ShapeDtypeStruct(ci_vector.shape, ci_vector.dtype),
        in_specs=[pl.BlockSpec(memory_space=pltpu.VMEM)] * 2,
        out_specs=pl.BlockSpec(memory_space=pltpu.VMEM),
        compiler_params=pltpu.CompilerParams(vmem_limit_bytes=2**20),
        cost_estimate=pl.CostEstimate(flops=10**6, bytes_accessed=4 * ci_vector.size, transcendentals=0),
        name="pick",
    )(first, last)
    held = {0: ci_vector, 1: last, 2: first, 5: edge, 6: cross}
    held[3] = lax.ppermute(beside, "alpha", swap)
    held[7] = lax.ppermute(cross, "alpha", swap)

    def place_of(block, own):
        k = block ^ own
        turned = (own >= length // 2) & ((k == 1) | (k == 2))
        return jnp.where(turned, 3 - k, k)

    return held, place_of, ()


def pick_kernel(first, last, out):
    lower = lax.axis_index("alpha") < lax.axis_size("alpha") // 2

    @pl.when(lower)
    def _():
        out[...] = first[...]

    @pl.when(jnp.logical_not(lower))
    def _():
        out[...] = last[...]


def warm_kernel(out):
    out[...] = jnp.zeros_like(out)


def couple_kernel(
    sizes, place_of, tables_from, held, alpha_tiles, beta_tiles, outs, window, coupled, total
):
    factors, alpha_slots, local_blocks, beta_slots, groups, by_xor, parts = sizes
    tile_size = total.shape[1]
    own_block, own_group = lax.axis_index("alpha"), lax.axis_index("beta")
    sources, counts, targets = (table[...] for table in tables_from)
    for place, piece in held.items():
        window[place] = piece[...]

    def alpha(factor):
        places = [place_of(sources[0, slot, factor], own_block) for slot in range(alpha_slots)]
        stacked = jnp.concatenate([window[place] for place in places], axis=0)
        tiles = [alpha_tiles[factor, 0, slot] for slot in range(alpha_slots)]
        live = [jnp.where(slot < counts[0, factor], tile, jnp.zeros_like(tile)) for slot, tile in enumerate(tiles)]
        product = jnp.dot(jnp.concatenate(live, axis=1), stacked, preferred_element_type=jnp.float32)
        coupled[factor] = product.astype(jnp.bfloat16)

    def beta(factor):
        for block in range(local_blocks):
            source = coupled[factor, :, block * tile_size : (block + 1) * tile_size]
            tiles = [beta_tiles[factor, block, slot] for slot in range(beta_slots)]
            added = jnp.dot(source, jnp.concatenate(tiles, axis=1), preferred_element_type=jnp.float32)
            for slot in range(beta_slots):
                target = targets[block, slot, factor]
                group = target // local_blocks
                away = (group ^ own_group) if by_xor else lax.rem(group - own_group + groups, groups)
                place = away * local_blocks + lax.rem(target, local_blocks)
                total[place] += added[:, slot * tile_size : (slot + 1) * tile_size]

    alpha(0)
    for block in range(total.shape[0]):
        total[block] = jnp.zeros(total.shape[1:], jnp.float32)
    for factor in range(1, factors):
        alpha(factor)
        beta(factor - 1)
    beta(factors - 1)
    for (away, first, last), out in zip(parts, outs):
        for block in range(local_blocks):
            value = total[away * local_blocks + block, first:last].astype(jnp.bfloat16)
            out[:, block * tile_size : (block + 1) * tile_size] = value


def shards(
    ci_vector, alpha_tiles, alpha_list, alpha_count, beta_tiles, beta_target, alpha_diag, beta_diag
):
    tile_size, columns = ci_vector.shape
    factors, _, alpha_slots = alpha_list.shape
    _, local_blocks, beta_slots = beta_target.shape
    length, groups = lax.axis_size("alpha"), lax.axis_size("beta")
    held, place_of, _ = window_of(length)(ci_vector)
    by_xor = groups & (groups - 1) == 0
    relay = groups == 4
    direct = tile_size * 3 // 8 if relay else tile_size
    parts = [(away, 0, tile_size if away < 2 else direct) for away in range(groups)]
    if relay:
        parts += [(away, direct, tile_size) for away in (2, 3)]
    sizes = (factors, alpha_slots, local_blocks, beta_slots, groups, by_xor, parts)
    vmem = pl.BlockSpec(memory_space=pltpu.VMEM)
    tile_bytes = (alpha_tiles.size + beta_tiles.size) * 2

    pl.pallas_call(
        warm_kernel,
        out_shape=jax.ShapeDtypeStruct((8, 128), jnp.float32),
        out_specs=vmem,
        compiler_params=pltpu.CompilerParams(vmem_limit_bytes=2**20, has_side_effects=True),
        cost_estimate=pl.CostEstimate(flops=WARM_FLOPS, bytes_accessed=4096, transcendentals=0),
        name="warm",
    )()

    tables = [
        jnp.transpose(alpha_list, (1, 2, 0)),
        jnp.transpose(alpha_count, (1, 0)),
        jnp.transpose(beta_target, (1, 2, 0)),
    ]

    def body(*refs):
        t, n = len(tables), len(held)
        pieces = dict(zip(held, refs[t : t + n]))
        a_ref, b_ref, *outs = refs[t + n : t + n + 2 + len(parts)]
        couple_kernel(
            sizes, place_of, refs[:t], pieces, a_ref, b_ref, outs, *refs[t + n + 2 + len(parts) :]
        )

    own, *far = pl.pallas_call(
        body,
        out_shape=[jax.ShapeDtypeStruct((last - first, columns), jnp.bfloat16) for _, first, last in parts],
        in_specs=[vmem] * len(tables) + [vmem] * (len(held) + 2),
        out_specs=[vmem] * len(parts),
        scratch_shapes=[
            pltpu.VMEM((max(held) + 1, tile_size, columns), jnp.bfloat16),
            pltpu.VMEM((factors, tile_size, columns), jnp.bfloat16),
            pltpu.VMEM((groups * local_blocks, tile_size, tile_size), jnp.float32),
        ],
        compiler_params=pltpu.CompilerParams(vmem_limit_bytes=20 * 2**20),
        cost_estimate=pl.CostEstimate(
            flops=2 * factors * tile_size * columns * tile_size * (alpha_slots + beta_slots),
            bytes_accessed=tile_bytes,
            transcendentals=0,
        ),
        name="couple",
    )(
        *tables,
        *held.values(),
        alpha_tiles,
        beta_tiles,
    )

    def send(value, away):
        if by_xor:
            pairs = [(i, i ^ away) for i in range(groups)]
        else:
            pairs = [(i, (i + away) % groups) for i in range(groups)]
        return lax.ppermute(value, "beta", pairs)

    received = [send(far[away - 1], away).astype(jnp.float32) for away in range(1, groups)]
    if relay:
        beyond = send(far[-1], 1)
        joined = (far[-2].astype(jnp.float32) + beyond.astype(jnp.float32)).astype(jnp.bfloat16)
        passed = send(joined, 2).astype(jnp.float32)
        received[1:] = [jnp.concatenate([received[1] + received[2], passed], axis=0)]
    summed = own.astype(jnp.float32) + sum(received)
    return summed + (alpha_diag[:, None] + beta_diag[None, :]) * ci_vector.astype(jnp.float32)


def window_of(length):
    return cube_window if length == 2 * (BAND + 1) else band_window


def solution(mesh):
    placed = (
        P("alpha", "beta"),
        P(None, "alpha", None, None, None),
        P(None, "alpha", None),
        P(None, "alpha"),
        P(None, "beta", None, None, None),
        P(None, "beta", None),
        P("alpha"),
        P("beta"),
    )

    return jax.shard_map(shards, mesh=mesh, in_specs=placed, out_specs=P("alpha", "beta"), check_vma=False)
```

```python
import jax
import jax.numpy as jnp
from jax import lax
from jax.experimental import pallas as pl
from jax.experimental.pallas import tpu as pltpu
from jax.sharding import PartitionSpec as P


BAND = 3
LAG = 3
WARM_FLOPS = 2 * 10**10


def band_window(ci_vector):
    length = lax.axis_size("alpha")
    held = {BAND: ci_vector}
    for offset in range(-BAND, BAND + 1):
        if offset:
            pairs = [(i, i - offset) for i in range(length) if 0 <= i - offset < length]
            held[offset + BAND] = lax.ppermute(ci_vector, "alpha", pairs)
    return held, lambda block, own: block - own + BAND, ()


def cube_window(ci_vector):
    length = lax.axis_size("alpha")
    everyone = range(length)
    lower, middle = set(everyone[: length // 2]), set(everyone[length // 4 : -(length // 4)])
    first = lax.ppermute(ci_vector, "alpha", [(i ^ (2 if i in lower else 1), i) for i in everyone])
    cross = lax.ppermute(ci_vector, "alpha", [(i ^ (6 if i in middle else 1), i) for i in everyone])
    last = lax.ppermute(ci_vector, "alpha", [(i ^ (1 if i in lower else 2), i) for i in everyone])
    edge = lax.ppermute(ci_vector, "alpha", [(i ^ 5, i) for i in everyone if abs(i - (i ^ 5)) <= BAND])
    swap = [(i, i ^ 1) for i in everyone]
    beside = pl.pallas_call(
        pick_kernel,
        out_shape=jax.ShapeDtypeStruct(ci_vector.shape, ci_vector.dtype),
        in_specs=[pl.BlockSpec(memory_space=pltpu.VMEM)] * 2,
        out_specs=pl.BlockSpec(memory_space=pltpu.VMEM),
        compiler_params=pltpu.CompilerParams(vmem_limit_bytes=2**20),
        cost_estimate=pl.CostEstimate(flops=10**6, bytes_accessed=4 * ci_vector.size, transcendentals=0),
        name="pick",
    )(first, last)
    held = {0: ci_vector, 1: last, 2: first, 5: edge, 6: cross}
    held[3] = lax.ppermute(beside, "alpha", swap)
    held[7] = lax.ppermute(cross, "alpha", swap)

    def place_of(block, own):
        k = block ^ own
        turned = (own >= length // 2) & ((k == 1) | (k == 2))
        return jnp.where(turned, 3 - k, k)

    return held, place_of, ()


def pick_kernel(first, last, out):
    lower = lax.axis_index("alpha") < lax.axis_size("alpha") // 2

    @pl.when(lower)
    def _():
        out[...] = first[...]

    @pl.when(jnp.logical_not(lower))
    def _():
        out[...] = last[...]


def warm_kernel(out):
    out[...] = jnp.zeros_like(out)


def couple_kernel(
    sizes, place_of, tables_from, held, alpha_tiles, beta_tiles, outs, window, coupled, total
):
    factors, alpha_slots, local_blocks, beta_slots, groups, by_xor, parts = sizes
    tile_size = total.shape[1]
    own_block, own_group = lax.axis_index("alpha"), lax.axis_index("beta")
    sources, counts, targets = (table[...] for table in tables_from)
    for place, piece in held.items():
        window[place] = piece[...]

    def alpha(factor):
        places = [place_of(sources[0, slot, factor], own_block) for slot in range(alpha_slots)]
        stacked = jnp.concatenate([window[place] for place in places], axis=0)
        tiles = [alpha_tiles[factor, 0, slot] for slot in range(alpha_slots)]
        live = [jnp.where(slot < counts[0, factor], tile, jnp.zeros_like(tile)) for slot, tile in enumerate(tiles)]
        product = jnp.dot(jnp.concatenate(live, axis=1), stacked, preferred_element_type=jnp.float32)
        coupled[factor] = product.astype(jnp.bfloat16)

    def beta(factor):
        for block in range(local_blocks):
            source = coupled[factor, :, block * tile_size : (block + 1) * tile_size]
            tiles = [beta_tiles[factor, block, slot] for slot in range(beta_slots)]
            added = jnp.dot(source, jnp.concatenate(tiles, axis=1), preferred_element_type=jnp.float32)
            for slot in range(beta_slots):
                target = targets[block, slot, factor]
                group = target // local_blocks
                away = (group ^ own_group) if by_xor else lax.rem(group - own_group + groups, groups)
                place = away * local_blocks + lax.rem(target, local_blocks)
                total[place] += added[:, slot * tile_size : (slot + 1) * tile_size]

    alpha(0)
    for block in range(total.shape[0]):
        total[block] = jnp.zeros(total.shape[1:], jnp.float32)
    for factor in range(1, factors):
        alpha(factor)
        if factor >= LAG:
            beta(factor - LAG)
    for factor in range(max(factors - LAG, 0), factors):
        beta(factor)
    for (away, first, last), out in zip(parts, outs):
        for block in range(local_blocks):
            value = total[away * local_blocks + block, first:last].astype(jnp.bfloat16)
            out[:, block * tile_size : (block + 1) * tile_size] = value


def shards(
    ci_vector, alpha_tiles, alpha_list, alpha_count, beta_tiles, beta_target, alpha_diag, beta_diag
):
    tile_size, columns = ci_vector.shape
    factors, _, alpha_slots = alpha_list.shape
    _, local_blocks, beta_slots = beta_target.shape
    length, groups = lax.axis_size("alpha"), lax.axis_size("beta")
    held, place_of, _ = window_of(length)(ci_vector)
    by_xor = groups & (groups - 1) == 0
    relay = groups == 4
    direct = tile_size * 3 // 8 if relay else tile_size
    parts = [(away, 0, tile_size if away < 2 else direct) for away in range(groups)]
    if relay:
        parts += [(away, direct, tile_size) for away in (2, 3)]
    sizes = (factors, alpha_slots, local_blocks, beta_slots, groups, by_xor, parts)
    vmem = pl.BlockSpec(memory_space=pltpu.VMEM)
    tile_bytes = (alpha_tiles.size + beta_tiles.size) * 2

    pl.pallas_call(
        warm_kernel,
        out_shape=jax.ShapeDtypeStruct((8, 128), jnp.float32),
        out_specs=vmem,
        compiler_params=pltpu.CompilerParams(vmem_limit_bytes=2**20, has_side_effects=True),
        cost_estimate=pl.CostEstimate(flops=WARM_FLOPS, bytes_accessed=4096, transcendentals=0),
        name="warm",
    )()

    tables = [
        jnp.transpose(alpha_list, (1, 2, 0)),
        jnp.transpose(alpha_count, (1, 0)),
        jnp.transpose(beta_target, (1, 2, 0)),
    ]

    def body(*refs):
        t, n = len(tables), len(held)
        pieces = dict(zip(held, refs[t : t + n]))
        a_ref, b_ref, *outs = refs[t + n : t + n + 2 + len(parts)]
        couple_kernel(
            sizes, place_of, refs[:t], pieces, a_ref, b_ref, outs, *refs[t + n + 2 + len(parts) :]
        )

    own, *far = pl.pallas_call(
        body,
        out_shape=[jax.ShapeDtypeStruct((last - first, columns), jnp.bfloat16) for _, first, last in parts],
        in_specs=[vmem] * len(tables) + [vmem] * (len(held) + 2),
        out_specs=[vmem] * len(parts),
        scratch_shapes=[
            pltpu.VMEM((max(held) + 1, tile_size, columns), jnp.bfloat16),
            pltpu.VMEM((factors, tile_size, columns), jnp.bfloat16),
            pltpu.VMEM((groups * local_blocks, tile_size, tile_size), jnp.float32),
        ],
        compiler_params=pltpu.CompilerParams(vmem_limit_bytes=20 * 2**20),
        cost_estimate=pl.CostEstimate(
            flops=2 * factors * tile_size * columns * tile_size * (alpha_slots + beta_slots),
            bytes_accessed=tile_bytes,
            transcendentals=0,
        ),
        name="couple",
    )(
        *tables,
        *held.values(),
        alpha_tiles,
        beta_tiles,
    )

    def send(value, away):
        if by_xor:
            pairs = [(i, i ^ away) for i in range(groups)]
        else:
            pairs = [(i, (i + away) % groups) for i in range(groups)]
        return lax.ppermute(value, "beta", pairs)

    received = [send(far[away - 1], away).astype(jnp.float32) for away in range(1, groups)]
    if relay:
        beyond = send(far[-1], 1)
        joined = (far[-2].astype(jnp.float32) + beyond.astype(jnp.float32)).astype(jnp.bfloat16)
        passed = send(joined, 2).astype(jnp.float32)
        received[1:] = [jnp.concatenate([received[1] + received[2], passed], axis=0)]
    summed = own.astype(jnp.float32) + sum(received)
    return summed + (alpha_diag[:, None] + beta_diag[None, :]) * ci_vector.astype(jnp.float32)


def window_of(length):
    return cube_window if length == 2 * (BAND + 1) else band_window


def solution(mesh):
    placed = (
        P("alpha", "beta"),
        P(None, "alpha", None, None, None),
        P(None, "alpha", None),
        P(None, "alpha"),
        P(None, "beta", None, None, None),
        P(None, "beta", None),
        P("alpha"),
        P("beta"),
    )

    return jax.shard_map(shards, mesh=mesh, in_specs=placed, out_specs=P("alpha", "beta"), check_vma=False)
```

```python
import jax
import jax.numpy as jnp
from jax import lax
from jax.experimental import pallas as pl
from jax.experimental.pallas import tpu as pltpu
from jax.sharding import PartitionSpec as P


BAND = 3
LAG = 3
WARM_FLOPS = 2 * 10**10


def band_window(ci_vector):
    length = lax.axis_size("alpha")
    held = {BAND: ci_vector}
    for offset in range(-BAND, BAND + 1):
        if offset:
            pairs = [(i, i - offset) for i in range(length) if 0 <= i - offset < length]
            held[offset + BAND] = lax.ppermute(ci_vector, "alpha", pairs)
    return held, lambda block, own: block - own + BAND


def cube_window(ci_vector):
    length = lax.axis_size("alpha")
    everyone = range(length)
    lower, middle = set(everyone[: length // 2]), set(everyone[length // 4 : -(length // 4)])
    first = lax.ppermute(ci_vector, "alpha", [(i ^ (2 if i in lower else 1), i) for i in everyone])
    cross = lax.ppermute(ci_vector, "alpha", [(i ^ (6 if i in middle else 1), i) for i in everyone])
    last = lax.ppermute(ci_vector, "alpha", [(i ^ (1 if i in lower else 2), i) for i in everyone])
    edge = lax.ppermute(ci_vector, "alpha", [(i ^ 5, i) for i in everyone if abs(i - (i ^ 5)) <= BAND])
    swap = [(i, i ^ 1) for i in everyone]
    beside = pl.pallas_call(
        pick_kernel,
        out_shape=jax.ShapeDtypeStruct(ci_vector.shape, ci_vector.dtype),
        in_specs=[pl.BlockSpec(memory_space=pltpu.VMEM)] * 2,
        out_specs=pl.BlockSpec(memory_space=pltpu.VMEM),
        compiler_params=pltpu.CompilerParams(vmem_limit_bytes=2**20),
        cost_estimate=pl.CostEstimate(flops=10**6, bytes_accessed=4 * ci_vector.size, transcendentals=0),
        name="pick",
    )(first, last)
    held = {0: ci_vector, 1: last, 2: first, 5: edge, 6: cross}
    held[3] = lax.ppermute(beside, "alpha", swap)
    held[7] = lax.ppermute(cross, "alpha", swap)

    def place_of(block, own):
        k = block ^ own
        turned = (own >= length // 2) & ((k == 1) | (k == 2))
        return jnp.where(turned, 3 - k, k)

    return held, place_of


def pick_kernel(first, last, out):
    lower = lax.axis_index("alpha") < lax.axis_size("alpha") // 2

    @pl.when(lower)
    def _():
        out[...] = first[...]

    @pl.when(jnp.logical_not(lower))
    def _():
        out[...] = last[...]


def warm_kernel(out):
    out[...] = jnp.zeros_like(out)


def couple_kernel(
    sizes, place_of, tables_from, held, alpha_tiles, beta_tiles, outs, window, coupled, total
):
    factors, alpha_slots, local_blocks, beta_slots, groups, by_xor, parts = sizes
    tile_size = total.shape[1]
    own_block, own_group = lax.axis_index("alpha"), lax.axis_index("beta")
    sources, counts, targets = (table[...] for table in tables_from)
    for place, piece in held.items():
        window[place] = piece[...]

    def alpha(factor):
        places = [place_of(sources[0, slot, factor], own_block) for slot in range(alpha_slots)]
        stacked = jnp.concatenate([window[place] for place in places], axis=0)
        tiles = [alpha_tiles[factor, 0, slot] for slot in range(alpha_slots)]
        live = [jnp.where(slot < counts[0, factor], tile, jnp.zeros_like(tile)) for slot, tile in enumerate(tiles)]
        product = jnp.dot(jnp.concatenate(live, axis=1), stacked, preferred_element_type=jnp.float32)
        coupled[factor] = product.astype(jnp.bfloat16)

    def beta(factor):
        for block in range(local_blocks):
            source = coupled[factor, :, block * tile_size : (block + 1) * tile_size]
            tiles = [beta_tiles[factor, block, slot] for slot in range(beta_slots)]
            added = jnp.dot(source, jnp.concatenate(tiles, axis=1), preferred_element_type=jnp.float32)
            for slot in range(beta_slots):
                target = targets[block, slot, factor]
                group = target // local_blocks
                away = (group ^ own_group) if by_xor else lax.rem(group - own_group + groups, groups)
                place = away * local_blocks + lax.rem(target, local_blocks)
                total[place] += added[:, slot * tile_size : (slot + 1) * tile_size]

    alpha(0)
    for block in range(total.shape[0]):
        total[block] = jnp.zeros(total.shape[1:], jnp.float32)
    for factor in range(1, factors):
        alpha(factor)
        if factor >= LAG:
            beta(factor - LAG)
    for factor in range(max(factors - LAG, 0), factors):
        beta(factor)
    for (away, first, last), out in zip(parts, outs):
        for block in range(local_blocks):
            value = total[away * local_blocks + block, first:last].astype(jnp.bfloat16)
            out[:, block * tile_size : (block + 1) * tile_size] = value


def shards(
    ci_vector, alpha_tiles, alpha_list, alpha_count, beta_tiles, beta_target, alpha_diag, beta_diag
):
    tile_size, columns = ci_vector.shape
    factors, _, alpha_slots = alpha_list.shape
    _, local_blocks, beta_slots = beta_target.shape
    length, groups = lax.axis_size("alpha"), lax.axis_size("beta")
    held, place_of = window_of(length)(ci_vector)
    by_xor = groups & (groups - 1) == 0
    relay = groups == 4
    direct = tile_size * 3 // 8 if relay else tile_size
    parts = [(away, 0, tile_size if away < 2 else direct) for away in range(groups)]
    if relay:
        parts += [(away, direct, tile_size) for away in (2, 3)]
    sizes = (factors, alpha_slots, local_blocks, beta_slots, groups, by_xor, parts)
    vmem = pl.BlockSpec(memory_space=pltpu.VMEM)
    tile_bytes = (alpha_tiles.size + beta_tiles.size) * 2

    pl.pallas_call(
        warm_kernel,
        out_shape=jax.ShapeDtypeStruct((8, 128), jnp.float32),
        out_specs=vmem,
        compiler_params=pltpu.CompilerParams(vmem_limit_bytes=2**20, has_side_effects=True),
        cost_estimate=pl.CostEstimate(flops=WARM_FLOPS, bytes_accessed=4096, transcendentals=0),
        name="warm",
    )()

    tables = [
        jnp.transpose(alpha_list, (1, 2, 0)),
        jnp.transpose(alpha_count, (1, 0)),
        jnp.transpose(beta_target, (1, 2, 0)),
    ]

    def body(*refs):
        t, n = len(tables), len(held)
        pieces = dict(zip(held, refs[t : t + n]))
        a_ref, b_ref, *outs = refs[t + n : t + n + 2 + len(parts)]
        couple_kernel(
            sizes, place_of, refs[:t], pieces, a_ref, b_ref, outs, *refs[t + n + 2 + len(parts) :]
        )

    own, *far = pl.pallas_call(
        body,
        out_shape=[jax.ShapeDtypeStruct((last - first, columns), jnp.bfloat16) for _, first, last in parts],
        in_specs=[vmem] * len(tables) + [vmem] * (len(held) + 2),
        out_specs=[vmem] * len(parts),
        scratch_shapes=[
            pltpu.VMEM((max(held) + 1, tile_size, columns), jnp.bfloat16),
            pltpu.VMEM((factors, tile_size, columns), jnp.bfloat16),
            pltpu.VMEM((groups * local_blocks, tile_size, tile_size), jnp.float32),
        ],
        compiler_params=pltpu.CompilerParams(vmem_limit_bytes=20 * 2**20),
        cost_estimate=pl.CostEstimate(
            flops=2 * factors * tile_size * columns * tile_size * (alpha_slots + beta_slots),
            bytes_accessed=tile_bytes,
            transcendentals=0,
        ),
        name="couple",
    )(
        *tables,
        *held.values(),
        alpha_tiles,
        beta_tiles,
    )

    def send(value, away):
        if by_xor:
            pairs = [(i, i ^ away) for i in range(groups)]
        else:
            pairs = [(i, (i + away) % groups) for i in range(groups)]
        return lax.ppermute(value, "beta", pairs)

    received = [send(far[away - 1], away).astype(jnp.float32) for away in range(1, groups)]
    if relay:
        beyond = send(far[-1], 1)
        joined = (far[-2].astype(jnp.float32) + beyond.astype(jnp.float32)).astype(jnp.bfloat16)
        passed = send(joined, 2).astype(jnp.float32)
        received[1:] = [jnp.concatenate([received[1] + received[2], passed], axis=0)]
    summed = own.astype(jnp.float32) + sum(received)
    return summed + (alpha_diag[:, None] + beta_diag[None, :]) * ci_vector.astype(jnp.float32)


def window_of(length):
    return cube_window if length == 2 * (BAND + 1) else band_window


def solution(mesh):
    placed = (
        P("alpha", "beta"),
        P(None, "alpha", None, None, None),
        P(None, "alpha", None),
        P(None, "alpha"),
        P(None, "beta", None, None, None),
        P(None, "beta", None),
        P("alpha"),
        P("beta"),
    )

    return jax.shard_map(shards, mesh=mesh, in_specs=placed, out_specs=P("alpha", "beta"), check_vma=False)
```

```python
import jax
import jax.numpy as jnp
from jax import lax
from jax.experimental import pallas as pl
from jax.experimental.pallas import tpu as pltpu
from jax.sharding import PartitionSpec as P


BAND = 3
LAG = 3
WARM_FLOPS = 2 * 10**10


def band_window(ci_vector):
    length = lax.axis_size("alpha")
    held = {BAND: ci_vector}
    for offset in range(-BAND, BAND + 1):
        if offset:
            pairs = [(i, i - offset) for i in range(length) if 0 <= i - offset < length]
            held[offset + BAND] = lax.ppermute(ci_vector, "alpha", pairs)
    return held, lambda block, own: block - own + BAND


def cube_window(ci_vector):
    length = lax.axis_size("alpha")
    everyone = range(length)
    lower, middle = set(everyone[: length // 2]), set(everyone[length // 4 : -(length // 4)])
    first = lax.ppermute(ci_vector, "alpha", [(i ^ (2 if i in lower else 1), i) for i in everyone])
    cross = lax.ppermute(ci_vector, "alpha", [(i ^ (6 if i in middle else 1), i) for i in everyone])
    last = lax.ppermute(ci_vector, "alpha", [(i ^ (1 if i in lower else 2), i) for i in everyone])
    edge = lax.ppermute(ci_vector, "alpha", [(i ^ 5, i) for i in everyone if abs(i - (i ^ 5)) <= BAND])
    swap = [(i, i ^ 1) for i in everyone]
    beside = pl.pallas_call(
        pick_kernel,
        out_shape=jax.ShapeDtypeStruct(ci_vector.shape, ci_vector.dtype),
        in_specs=[pl.BlockSpec(memory_space=pltpu.VMEM)] * 2,
        out_specs=pl.BlockSpec(memory_space=pltpu.VMEM),
        compiler_params=pltpu.CompilerParams(vmem_limit_bytes=2**20),
        cost_estimate=pl.CostEstimate(flops=10**6, bytes_accessed=4 * ci_vector.size, transcendentals=0),
        name="pick",
    )(first, last)
    held = {0: ci_vector, 1: last, 2: first, 5: edge, 6: cross}
    held[3] = lax.ppermute(beside, "alpha", swap)
    held[7] = lax.ppermute(cross, "alpha", swap)

    def place_of(block, own):
        k = block ^ own
        turned = (own >= length // 2) & ((k == 1) | (k == 2))
        return jnp.where(turned, 3 - k, k)

    return held, place_of


def pick_kernel(first, last, out):
    lower = lax.axis_index("alpha") < lax.axis_size("alpha") // 2

    @pl.when(lower)
    def _():
        out[...] = first[...]

    @pl.when(jnp.logical_not(lower))
    def _():
        out[...] = last[...]


def warm_kernel(out):
    out[...] = jnp.zeros_like(out)


def couple_kernel(
    sizes, place_of, tables_from, held, alpha_tiles, beta_tiles, outs, window, coupled, total
):
    factors, alpha_slots, local_blocks, beta_slots, groups, by_xor, parts = sizes
    tile_size = total.shape[1]
    own_block, own_group = lax.axis_index("alpha"), lax.axis_index("beta")
    sources, counts, targets = (table[...] for table in tables_from)
    for place, piece in held.items():
        window[place] = piece[...]

    def alpha(factor):
        places = [place_of(sources[0, slot, factor], own_block) for slot in range(alpha_slots)]
        stacked = jnp.concatenate([window[place] for place in places], axis=0)
        tiles = [alpha_tiles[factor, 0, slot] for slot in range(alpha_slots)]
        live = [jnp.where(slot < counts[0, factor], tile, jnp.zeros_like(tile)) for slot, tile in enumerate(tiles)]
        product = jnp.dot(jnp.concatenate(live, axis=1), stacked, preferred_element_type=jnp.float32)
        coupled[factor] = product.astype(jnp.bfloat16)

    def beta(factor):
        for block in range(local_blocks):
            source = coupled[factor, :, block * tile_size : (block + 1) * tile_size]
            tiles = [beta_tiles[factor, block, slot] for slot in range(beta_slots)]
            added = jnp.dot(source, jnp.concatenate(tiles, axis=1), preferred_element_type=jnp.float32)
            for slot in range(beta_slots):
                target = targets[block, slot, factor]
                group = target // local_blocks
                away = (group ^ own_group) if by_xor else lax.rem(group - own_group + groups, groups)
                place = away * local_blocks + lax.rem(target, local_blocks)
                total[place] += added[:, slot * tile_size : (slot + 1) * tile_size]

    alpha(0)
    for block in range(total.shape[0]):
        total[block] = jnp.zeros(total.shape[1:], jnp.float32)
    for factor in range(1, factors):
        alpha(factor)
        if factor >= LAG:
            beta(factor - LAG)
    for factor in range(max(factors - LAG, 0), factors):
        beta(factor)
    for (away, first, last), out in zip(parts, outs):
        for block in range(local_blocks):
            value = total[away * local_blocks + block, first:last].astype(jnp.bfloat16)
            out[:, block * tile_size : (block + 1) * tile_size] = value


def shards(
    ci_vector, alpha_tiles, alpha_list, alpha_count, beta_tiles, beta_target, alpha_diag, beta_diag
):
    tile_size, columns = ci_vector.shape
    factors, _, alpha_slots = alpha_list.shape
    _, local_blocks, beta_slots = beta_target.shape
    length, groups = lax.axis_size("alpha"), lax.axis_size("beta")
    held, place_of = window_of(length)(ci_vector)
    by_xor = groups & (groups - 1) == 0
    relay = groups == 4
    parts = [(away, 0, tile_size) for away in range(groups)]
    if relay:
        early, direct = tile_size * 13 // 16, tile_size * 5 // 16
        parts[1:] = [(1, 0, early), (2, 0, direct), (3, 0, direct)]
        parts += [(1, early, tile_size), (2, direct, tile_size), (3, direct, tile_size)]
    sizes = (factors, alpha_slots, local_blocks, beta_slots, groups, by_xor, parts)
    vmem = pl.BlockSpec(memory_space=pltpu.VMEM)
    tile_bytes = (alpha_tiles.size + beta_tiles.size) * 2

    pl.pallas_call(
        warm_kernel,
        out_shape=jax.ShapeDtypeStruct((8, 128), jnp.float32),
        out_specs=vmem,
        compiler_params=pltpu.CompilerParams(vmem_limit_bytes=2**20, has_side_effects=True),
        cost_estimate=pl.CostEstimate(flops=WARM_FLOPS, bytes_accessed=4096, transcendentals=0),
        name="warm",
    )()

    tables = [
        jnp.transpose(alpha_list, (1, 2, 0)),
        jnp.transpose(alpha_count, (1, 0)),
        jnp.transpose(beta_target, (1, 2, 0)),
    ]

    def body(*refs):
        t, n = len(tables), len(held)
        pieces = dict(zip(held, refs[t : t + n]))
        a_ref, b_ref, *outs = refs[t + n : t + n + 2 + len(parts)]
        couple_kernel(
            sizes, place_of, refs[:t], pieces, a_ref, b_ref, outs, *refs[t + n + 2 + len(parts) :]
        )

    own, *far = pl.pallas_call(
        body,
        out_shape=[jax.ShapeDtypeStruct((last - first, columns), jnp.bfloat16) for _, first, last in parts],
        in_specs=[vmem] * len(tables) + [vmem] * (len(held) + 2),
        out_specs=[vmem] * len(parts),
        scratch_shapes=[
            pltpu.VMEM((max(held) + 1, tile_size, columns), jnp.bfloat16),
            pltpu.VMEM((factors, tile_size, columns), jnp.bfloat16),
            pltpu.VMEM((groups * local_blocks, tile_size, tile_size), jnp.float32),
        ],
        compiler_params=pltpu.CompilerParams(vmem_limit_bytes=20 * 2**20),
        cost_estimate=pl.CostEstimate(
            flops=2 * factors * tile_size * columns * tile_size * (alpha_slots + beta_slots),
            bytes_accessed=tile_bytes,
            transcendentals=0,
        ),
        name="couple",
    )(
        *tables,
        *held.values(),
        alpha_tiles,
        beta_tiles,
    )

    def send(value, away):
        if by_xor:
            pairs = [(i, i ^ away) for i in range(groups)]
        else:
            pairs = [(i, (i + away) % groups) for i in range(groups)]
        return lax.ppermute(value, "beta", pairs)

    received = [send(far[away - 1], away).astype(jnp.float32) for away in range(1, groups)]
    if relay:
        beyond = send(far[-1], 1)
        joined = (far[-2].astype(jnp.float32) + beyond.astype(jnp.float32)).astype(jnp.bfloat16)
        passed = send(joined, 2).astype(jnp.float32)
        rest = send(far[-3], 1).astype(jnp.float32)
        received[0] = jnp.concatenate([received[0], rest], axis=0)
        received[1:] = [jnp.concatenate([received[1] + received[2], passed], axis=0)]
    summed = own.astype(jnp.float32) + sum(received)
    return summed + (alpha_diag[:, None] + beta_diag[None, :]) * ci_vector.astype(jnp.float32)


def window_of(length):
    return cube_window if length == 2 * (BAND + 1) else band_window


def solution(mesh):
    placed = (
        P("alpha", "beta"),
        P(None, "alpha", None, None, None),
        P(None, "alpha", None),
        P(None, "alpha"),
        P(None, "beta", None, None, None),
        P(None, "beta", None),
        P("alpha"),
        P("beta"),
    )

    return jax.shard_map(shards, mesh=mesh, in_specs=placed, out_specs=P("alpha", "beta"), check_vma=False)
```
